32 devices in a mesh: ep: 16 (over z, y, x), opt: 2 (over core).
Axes of the slice: x: 2, y: 2, z: 4, core: 2. Of those that a mesh axis runs over, the one named last changes fastest.
Arguments:
- tokens: bfloat16 [2048, 2048], P('ep'), may hold values from -6 to 6
- out_grad: bfloat16 [2048, 2048], P('ep'), may hold values from -6 to 6
- expert_ids: int32 [2048, 2], P('ep'), may hold values from 0 to 15, all different within a row; in each aligned block of 128 rows (0 to 127, 128 to 255, ...) at most 32 rows name the same one
- route_gates: float32 [2048, 2], P('ep'), may hold values from 0.1 to 1
- gate_weight: bfloat16 [16, 2048, 512], P('ep', None, 'opt'), may hold values from -0.125 to 0.125
- up_weight: bfloat16 [16, 2048, 512], P('ep', None, 'opt'), may hold values from -0.125 to 0.125
- down_weight: bfloat16 [16, 512, 2048], P('ep', 'opt'), may hold values from -0.25 to 0.25
- momentum: float32 [16, 512, 2048], P('ep', 'opt'), may hold values from -80 to 80
Outputs:
- token_grad: bfloat16 [2048, 2048], P('ep', 'opt')
- new_momentum: float32 [16, 512, 2048], P('ep', 'opt')
- update: float32 [16, 512, 2048], P('ep', 'opt')
The draws below stay inside these ranges and needn't reach their ends.
Inputs may be any that keep to these rules, and one draw needn't show every extreme that they name: `expert_ids`: within the rows of one index of ep, each expert is named at most 32 times, a bound that some block reaches; the 2 ids of a token differ.
All inputs are finite; a program needn't handle non-finite values.
Results may differ from the reference program's by a relative error of at most 0.011.
Values may be sent and summed in bfloat16 or wider, within the bound.
A program may use at most 64 MiB of HBM per device.

```python
import math
import jax
import jax.numpy as jnp
import numpy as np
from jax import lax

D = 2048
FF = 512
TOK_DEV = 128
TOPK = 2
NS_ITERS = 3
EXPERTS = 16
CAP = 32
TOKENS = 2048
N_EP = 16


def draw_momentum(key, part):
    subkeys = jax.random.split(key, 2)
    row_frac = jnp.arange(FF).astype(jnp.float32) / FF
    row_scale = jnp.power(10.0, row_frac)[None, :, None]
    col_scale = jnp.exp(jax.random.uniform(subkeys[1], (EXPERTS, 1, D), jnp.float32) * jnp.log(10.0))
    values = jnp.clip(jax.random.normal(subkeys[0], (EXPERTS, FF, D), jnp.float32), -4.0, 4.0)
    return jnp.clip(0.2 * values * row_scale * col_scale, -80.0, 80.0)


def block_scale(key, dims, cuts, smallest, high):
    gain, own = 1.0, jax.random.fold_in(key, 6)
    for axis_at, blocks in cuts:
        heights = jnp.exp(jax.random.uniform(jax.random.fold_in(own, axis_at), (blocks,), jnp.float32, smallest / len(cuts), high / len(cuts)))
        gain = gain * jnp.repeat(heights, dims[axis_at] // blocks).reshape([-1 if axis == axis_at else 1 for axis in range(len(dims))])
    return gain


def deal_out(own_key, own, number, rows, count, top, bound, slope):
    sequence = jax.random.permutation(own_key, count)
    crowded, usual = load_shares(count, rows * top, bound, slope, True), load_shares(count, rows * top, bound, slope, False)
    places = jnp.arange(count)

    def named(lengths, offset_by):
        used = int((lengths > 0).sum())
        fixed = max(1, used // 4)
        moved = fixed + (places - fixed + offset_by * (used - fixed)) % max(1, count - fixed)
        return jnp.zeros((count,), jnp.int32).at[sequence[jnp.where(places < fixed, places, moved)]].set(jnp.asarray(lengths, jnp.int32))

    lengths = jnp.where(number % 4 == 0, named(crowded, number // 4), named(usual, number - number // 4 - 1))
    mixed = jax.random.permutation(jax.random.fold_in(own, 3), count)
    giver, sink = mixed[0:count // 2 * 2:2], mixed[1:count // 2 * 2:2]
    slack = jnp.minimum(lengths[giver] - 1, bound - lengths[sink]) // 2
    slack = jnp.where((giver == sequence[0]) | (sink == sequence[0]) | (lengths[sink] == 0), 0, jnp.maximum(slack, 0))
    moved = jax.random.randint(jax.random.fold_in(own, 4), (count // 2,), 0, 1 << 20) % (slack + 1)
    lengths = lengths.at[giver].add(-moved).at[sink].add(moved)
    members = jnp.searchsorted(jnp.cumsum(lengths), jnp.arange(rows * top), side="right").astype(jnp.int32)
    table = members.reshape(top, rows).T
    table = table[jax.random.permutation(jax.random.fold_in(own, 1), rows)]
    offset_by = jax.random.randint(jax.random.fold_in(own, 2), (rows, 1), 0, top)
    return jnp.take_along_axis(table, (jnp.arange(top)[None, :] + offset_by) % top, axis=1)


def load_shares(number_of, total, most, skew, full):
    weights = [(1 << 20) // math.isqrt(standing ** skew) + 1 for standing in range(1, number_of + 1)]
    largest = most if full else min(most, max(-(-total // number_of), total * weights[0] // sum(weights)))
    least = 1 if total - largest >= number_of - 1 else 0
    given, surplus = [largest] + [least] * (number_of - 1), total - largest - least * (number_of - 1)
    while surplus > 0:
        free = [i for i in range(1, number_of) if given[i] < largest] or [i for i in range(1, number_of) if given[i] < most]
        whole, budget = sum([weights[i] for i in free]), surplus
        for i in free:
            more = min(most - given[i], max(1, budget * weights[i] // whole), surplus)
            given[i] = given[i] + more
            surplus = surplus - more
    return np.array(given)


def scatter_about(key, dims, deviation, bound, pieces=(), kind=jnp.bfloat16):
    values = deviation * jax.random.normal(key, dims, jnp.float32)
    if pieces:
        values = values * block_scale(key, dims, pieces, -0.22, 0.18)
    return jnp.clip(values, -bound, bound).astype(kind)


def setup_inputs(seed: int = 0) -> dict:
    splits = jax.random.split(jax.random.key(seed), 9)
    tokens = scatter_about(splits[0], (TOKENS, D), 1.0, 6.0, ((0, 16),))
    out_grad = scatter_about(splits[1], (TOKENS, D), 1.0, 6.0, ((0, 16),))
    expert_ids_keys = jax.random.split(jax.random.fold_in(splits[2], 1), TOKENS // TOK_DEV)
    expert_ids_turns = jax.random.permutation(jax.random.fold_in(splits[2], 3), TOKENS // TOK_DEV)
    expert_ids = jax.vmap(lambda own, number: deal_out(jax.random.fold_in(splits[2], 2), own, number, TOK_DEV, EXPERTS, TOPK, CAP, 2))(expert_ids_keys, expert_ids_turns).reshape((TOKENS, TOPK))
    route_gates = jnp.clip(0.1 + 0.9 * jax.random.uniform(splits[3], (TOKENS, TOPK), jnp.float32) ** block_scale(splits[3], (TOKENS, TOPK), ((0, 16),), -0.2, 0.2), 0.1, 1.0)
    gate_weight = scatter_about(splits[4], (EXPERTS, D, FF), D ** -0.5, 0.125, ((0, 16), (2, 2)))
    up_weight = scatter_about(splits[5], (EXPERTS, D, FF), D ** -0.5, 0.125, ((0, 16), (2, 2)))
    down_weight = scatter_about(splits[6], (EXPERTS, FF, D), FF ** -0.5, 0.25, ((0, 16), (1, 2)))
    momentum = draw_momentum(jax.random.fold_in(splits[8], 71), 0)
    return dict(tokens=tokens, out_grad=out_grad, expert_ids=expert_ids, route_gates=route_gates, gate_weight=gate_weight, up_weight=up_weight, down_weight=down_weight, momentum=momentum)


momentum_decay = 0.95
coeff_one = 3.4445
coeff_two = -4.775
coeff_three = 2.0315
epsilon = 1e-07

def entry_rank(block_ids):
    experts_all = jnp.arange(EXPERTS, dtype=jnp.int32)
    onehot = (block_ids[:, None] == experts_all[None, :]).astype(jnp.int32)
    before = jnp.cumsum(onehot, axis=0) - onehot
    return lax.optimization_barrier(jnp.sum(before * onehot, axis=1)).astype(jnp.int32)

def newton_schulz(initial):
    orthogonal = initial
    for iteration in range(NS_ITERS):
        gram_matrix = jnp.dot(orthogonal, orthogonal.T, preferred_element_type=jnp.float32).astype(jnp.bfloat16)
        squared = jnp.dot(gram_matrix, gram_matrix, preferred_element_type=jnp.float32)
        polynomial = (coeff_two * gram_matrix.astype(jnp.float32) + coeff_three * squared).astype(jnp.bfloat16)
        product = jnp.dot(polynomial, orthogonal, preferred_element_type=jnp.float32)
        orthogonal = (coeff_one * orthogonal.astype(jnp.float32) + product).astype(jnp.bfloat16)
    return orthogonal

def reference(tokens, out_grad, expert_ids, route_gates, gate_weight, up_weight, down_weight, momentum):
    model_width = tokens.shape[1]
    flat_ids = expert_ids.reshape(N_EP, TOK_DEV * TOPK).astype(jnp.int32)
    ranks_all = jax.vmap(entry_rank)(flat_ids)
    source = jnp.arange(N_EP, dtype=jnp.int32)[:, None]
    entries = jnp.arange(TOK_DEV * TOPK, dtype=jnp.int32)[None, :]
    position = (flat_ids * (N_EP * CAP) + source * CAP + ranks_all).reshape(-1).astype(jnp.int32)
    token_index = (source * TOK_DEV + entries // TOPK).reshape(-1).astype(jnp.int32)
    slots_all = EXPERTS * N_EP * CAP
    slot_table = jnp.full((slots_all,), -1, jnp.int32).at[position].set(token_index)
    slot_table = slot_table.reshape(EXPERTS, N_EP * CAP)
    gate_table = jnp.zeros((slots_all,), jnp.float32).at[position].set(route_gates.reshape(-1))
    gate_table = gate_table.reshape(EXPERTS, N_EP * CAP)

    def expert_step(grad_sum, inputs):
        rows_index, row_gates, weight_gate, weight_up, weight_down, moment = inputs
        filled = rows_index >= 0
        safe_index = jnp.maximum(rows_index, 0).astype(jnp.int32)
        input_rows = jnp.where(filled[:, None], tokens[safe_index], jnp.zeros((), tokens.dtype))
        scaled = (row_gates[:, None] * out_grad[safe_index].astype(jnp.float32)).astype(jnp.bfloat16)
        pre_gate = jnp.dot(input_rows, weight_gate, preferred_element_type=jnp.float32)
        pre_up = jnp.dot(input_rows, weight_up, preferred_element_type=jnp.float32)
        sigmoid = jax.nn.sigmoid(pre_gate)
        activated = pre_gate * sigmoid
        hidden = (activated * pre_up).astype(jnp.bfloat16)
        hidden_grad = jnp.dot(scaled, weight_down.T, preferred_element_type=jnp.float32)
        gate_grad = (hidden_grad * pre_up * sigmoid * (1.0 + pre_gate * (1.0 - sigmoid))).astype(jnp.bfloat16)
        up_grad = (hidden_grad * activated).astype(jnp.bfloat16)
        row_grad = (jnp.dot(gate_grad, weight_gate.T, preferred_element_type=jnp.float32) + jnp.dot(up_grad, weight_up.T, preferred_element_type=jnp.float32)).astype(jnp.bfloat16)
        grad_sum = grad_sum.at[safe_index].add(jnp.where(filled[:, None], row_grad.astype(jnp.float32), 0.0))
        down_grad = jnp.dot(hidden.T, scaled, preferred_element_type=jnp.float32)
        new_moment = momentum_decay * moment + down_grad
        frob_norm = jnp.sqrt(jnp.sum(new_moment * new_moment))
        initial = (new_moment / (frob_norm + epsilon)).astype(jnp.bfloat16)
        result = newton_schulz(initial)
        update = math.sqrt(model_width) * result.astype(jnp.float32)
        return (grad_sum, (new_moment, update))
    start_sum = jnp.zeros((N_EP * TOK_DEV, model_width), jnp.float32)
    token_sum, outputs = lax.scan(expert_step, start_sum, (slot_table, gate_table, gate_weight, up_weight, down_weight, momentum))
    return (token_sum.astype(jnp.bfloat16), outputs[0], outputs[1])
```

```python
import functools
import math

import jax
import jax.numpy as jnp
from jax import lax
from jax.experimental import pallas as pl
from jax.experimental.pallas import tpu as pltpu
from jax.sharding import PartitionSpec as P

NS_ITERS = 3
MESH = pl.DeviceIdType.MESH

momentum_decay = 0.95
coeff_one = 3.4445
coeff_two = -4.775
coeff_three = 2.0315
epsilon = 1e-07

CONTRACT_LAST = (((1,), (1,)), ((), ()))
CONTRACT_FIRST = (((0,), (0,)), ((), ()))


def loop(count, body, start=0):
    def step(index, carry):
        body(index)
        return carry

    lax.fori_loop(start, count, step, 0)


def greet_all(peers, me, core):
    barrier = pltpu.get_barrier_semaphore()

    def greet(step):
        other = lax.rem(me + step, peers)
        pl.semaphore_signal(barrier, inc=1, device_id=(other, core), device_id_type=MESH)

    loop(peers, greet, 1)
    pl.semaphore_signal(barrier, inc=1, device_id=(me, 1 - core), device_id_type=MESH)
    pl.semaphore_wait(barrier, peers)


def dispatch_kernel(
    peers, send_first, send_second, out_first, out_second,
    local_sems, send_sems, recv_sems, push_sems, pull_sems,
):
    me, core = lax.axis_index("ep"), lax.axis_index("opt")
    part = send_first.shape[2]
    columns = pl.ds(pl.multiple_of(core * part, part), part)
    greet_all(peers, me, core)
    pairs = ((send_first, out_first), (send_second, out_second))

    def remote(which, other, source):
        send_ref, out_ref = pairs[which]
        return pltpu.make_async_remote_copy(
            src_ref=send_ref.at[other],
            dst_ref=out_ref.at[source, :, columns],
            send_sem=send_sems.at[which, other],
            recv_sem=recv_sems.at[which, source],
            device_id=(other, core),
            device_id_type=MESH,
        )

    def push(which, source, own):
        send_ref, out_ref = pairs[which]
        return pltpu.make_async_remote_copy(
            src_ref=send_ref.at[source] if own else out_ref.at[source, :, columns],
            dst_ref=out_ref.at[source, :, columns],
            send_sem=push_sems.at[which, source],
            recv_sem=pull_sems.at[which, source],
            device_id=(me, 1 - core),
            device_id_type=MESH,
        )

    other_columns = pl.ds(pl.multiple_of((1 - core) * part, part), part)

    def pull(which, source):
        out_ref = pairs[which][1]
        return pltpu.make_async_remote_copy(
            src_ref=out_ref.at[source, :, other_columns],
            dst_ref=out_ref.at[source, :, other_columns],
            send_sem=push_sems.at[which, source],
            recv_sem=pull_sems.at[which, source],
            device_id=(me, 1 - core),
            device_id_type=MESH,
        )

    for which in range(2):
        loop(peers, lambda step: remote(which, lax.rem(me + step, peers), me).start(), 1)
    for which in range(2):
        push(which, me, True).start()
        send_ref, out_ref = pairs[which]
        pltpu.make_async_copy(
            send_ref.at[me], out_ref.at[me, :, columns], local_sems.at[which]
        ).start()
    for which in range(2):

        def arrive(step):
            source = lax.rem(me + peers - step, peers)
            remote(which, source, source).wait_recv()
            push(which, source, False).start()

        loop(peers, arrive, 1)
    for which in range(2):
        send_ref, out_ref = pairs[which]
        pltpu.make_async_copy(
            send_ref.at[me], out_ref.at[me, :, columns], local_sems.at[which]
        ).wait()
        push(which, me, True).wait_send()

        def finish(step):
            source = lax.rem(me + peers - step, peers)
            remote(which, source, me).wait_send()
            push(which, source, False).wait_send()

        loop(peers, finish, 1)
        loop(peers, lambda source: pull(which, source).wait_recv())


def dispatch(send_first, send_second, peers, cores):
    _, rows, part = send_first.shape
    out = jax.ShapeDtypeStruct((peers, rows, part * cores), send_first.dtype)
    vmem = pl.BlockSpec(memory_space=pltpu.VMEM)
    sems = pltpu.SemaphoreType.DMA((2, peers))
    return pl.pallas_call(
        functools.partial(dispatch_kernel, peers),
        out_shape=(out, out),
        in_specs=[vmem] * 2,
        out_specs=(vmem, vmem),
        scratch_shapes=[pltpu.SemaphoreType.DMA((2,)), sems, sems, sems, sems],
        compiler_params=pltpu.CompilerParams(collective_id=0, has_side_effects=True),
        name="dispatch",
    )(send_first, send_second)


def return_kernel(
    peers, groups, partial, moment, squares, returned, ortho_out,
    extra, summed, other_squares, ortho, gram, gram_low, poly,
    send_sems, recv_sems, swap_send, swap_recv, misc_sems,
):
    me, core = lax.axis_index("ep"), lax.axis_index("opt")
    part = summed.shape[2]
    size = peers // groups
    own_rows, width = moment.shape
    all_rows = ortho.shape[0]
    own = pl.ds(pl.multiple_of(core * part, part), part)
    others = pl.ds(pl.multiple_of((1 - core) * part, part), part)
    greet_all(peers, me, core)
    mine = lax.div(me, size)

    def swap(step):
        first = lax.rem(mine + step, groups) * size
        return pltpu.make_async_remote_copy(
            src_ref=partial.at[pl.ds(first, size), :, others],
            dst_ref=extra.at[pl.ds(first, size)],
            send_sem=swap_send.at[step],
            recv_sem=swap_recv.at[step],
            device_id=(me, 1 - core),
            device_id_type=MESH,
        )

    def remote(other, source):
        return pltpu.make_async_remote_copy(
            src_ref=summed.at[other],
            dst_ref=returned.at[source],
            send_sem=send_sems.at[other],
            recv_sem=recv_sems.at[source],
            device_id=(other, core),
            device_id_type=MESH,
        )

    sums = pltpu.make_async_remote_copy(
        src_ref=squares,
        dst_ref=other_squares,
        send_sem=misc_sems.at[0],
        recv_sem=misc_sems.at[1],
        device_id=(me, 1 - core),
        device_id_type=MESH,
    )
    sums.start()
    loop(groups, lambda step: swap(step).start())
    sums.wait()
    frob = jnp.sqrt(squares[...] + other_squares[...])
    scale = (1.0 / (frob + epsilon))[0:1, 0:1]
    row_start = pl.multiple_of(core * own_rows, own_rows)
    row_tile = own_rows // 4

    def normalize(index):
        rows = pl.ds(pl.multiple_of(index * row_tile, row_tile), row_tile)
        target = pl.ds(pl.multiple_of(row_start + index * row_tile, row_tile), row_tile)
        ortho[target, :] = (moment[rows, :] * scale).astype(jnp.bfloat16)

    loop(4, normalize)

    def rows_copy(start):
        rows = pl.ds(pl.multiple_of(start, own_rows), own_rows)
        return pltpu.make_async_remote_copy(
            src_ref=ortho.at[rows],
            dst_ref=ortho.at[rows],
            send_sem=misc_sems.at[2],
            recv_sem=misc_sems.at[3],
            device_id=(me, 1 - core),
            device_id_type=MESH,
        )

    def leave(step):
        swap(step).wait_recv()
        first = lax.rem(mine + step, groups) * size

        def add(offset):
            other = first + offset
            total = partial[other, :, own].astype(jnp.float32) + extra[other].astype(jnp.float32)
            summed[other] = total.astype(jnp.bfloat16)

        def send(offset):
            other = first + offset

            @pl.when(other != me)
            def _():
                remote(other, me).start()

            @pl.when(other == me)
            def _():
                pltpu.make_async_copy(summed.at[me], returned.at[me], misc_sems.at[4]).start()

        loop(size, add)
        loop(size, send)

    loop(groups, leave)
    rows_copy(row_start).start()
    rows_copy((1 - core) * own_rows).wait_recv()
    rows_copy(row_start).wait_send()

    tile = min(512, width)
    tiles = width // tile

    def columns_of(index):
        return pl.ds(pl.multiple_of(index * tile, tile), tile)

    for iteration in range(NS_ITERS):
        gram[...] = jnp.zeros_like(gram)

        def grow(index):
            block = ortho[:, columns_of(index)]
            gram[...] += lax.dot_general(
                block, block, CONTRACT_LAST, preferred_element_type=jnp.float32
            )

        loop(tiles, grow)
        gram_low[...] = gram[...].astype(jnp.bfloat16)
        low = gram_low[...]
        squared = jnp.dot(low, low, preferred_element_type=jnp.float32)
        poly[...] = (coeff_two * low.astype(jnp.float32) + coeff_three * squared).astype(
            jnp.bfloat16
        )
        last = iteration == NS_ITERS - 1

        def apply(index):
            columns = columns_of(index)
            block = ortho[:, columns]
            if last:
                rows = pl.ds(row_start, own_rows)
                product = jnp.dot(poly[rows, :], block, preferred_element_type=jnp.float32)
                before = ortho[rows, columns].astype(jnp.float32)
                ortho_out[:, columns] = (coeff_one * before + product).astype(jnp.bfloat16)
            else:
                product = jnp.dot(poly[...], block, preferred_element_type=jnp.float32)
                ortho[:, columns] = (coeff_one * block.astype(jnp.float32) + product).astype(
                    jnp.bfloat16
                )

        loop(tiles, apply)

    pltpu.make_async_copy(summed.at[me], returned.at[me], misc_sems.at[4]).wait()

    def finish(step):
        other = lax.rem(me + step, peers)
        remote(other, me).wait_send()
        remote(other, other).wait_recv()

    loop(peers, finish, 1)
    loop(groups, lambda step: swap(step).wait_send())


def return_and_orthogonalize(partial, moment, squares, cores):
    peers, rows, width = partial.shape
    part = width // cores
    own_rows = moment.shape[0]
    all_rows = own_rows * cores
    groups = 4
    vmem = pl.BlockSpec(memory_space=pltpu.VMEM)
    dma = pltpu.SemaphoreType.DMA
    return pl.pallas_call(
        functools.partial(return_kernel, peers, groups),
        out_shape=(
            jax.ShapeDtypeStruct((peers, rows, part), jnp.bfloat16),
            jax.ShapeDtypeStruct((own_rows, width), jnp.bfloat16),
        ),
        in_specs=[vmem] * 3,
        out_specs=(vmem, vmem),
        scratch_shapes=[
            pltpu.VMEM((peers, rows, part), jnp.bfloat16),
            pltpu.VMEM((peers, rows, part), jnp.bfloat16),
            pltpu.VMEM(squares.shape, jnp.float32),
            pltpu.VMEM((all_rows, width), jnp.bfloat16),
            pltpu.VMEM((all_rows, all_rows), jnp.float32),
            pltpu.VMEM((all_rows, all_rows), jnp.bfloat16),
            pltpu.VMEM((all_rows, all_rows), jnp.bfloat16),
            dma((peers,)),
            dma((peers,)),
            dma((groups,)),
            dma((groups,)),
            dma((5,)),
        ],
        compiler_params=pltpu.CompilerParams(collective_id=1, has_side_effects=True),
        name="return_ortho",
    )(partial, moment, squares)


def placement(expert_ids, route_gates, slot_count, capacity):
    token_count, topk_count = expert_ids.shape
    earlier = (
        lax.broadcasted_iota(jnp.int32, (token_count, token_count), 0)
        < lax.broadcasted_iota(jnp.int32, (token_count, token_count), 1)
    )
    slot_iota = lax.broadcasted_iota(jnp.int32, (slot_count, token_count), 0)
    chosen = jnp.zeros((slot_count, token_count), jnp.bool_)
    gates = jnp.zeros((slot_count, token_count), jnp.float32)
    for k in range(topk_count):
        ids_row = expert_ids[:, k][None, :]
        same = jnp.zeros((token_count, token_count), jnp.bool_)
        for other in range(topk_count):
            same = same | (expert_ids[:, other][:, None] == ids_row)
        rank = jnp.sum((same & earlier).astype(jnp.int32), axis=0)
        hit = slot_iota == (expert_ids[:, k] * capacity + rank)[None, :]
        chosen = chosen | hit
        gates = gates + jnp.where(hit, route_gates[:, k][None, :], 0.0)
    return chosen.astype(jnp.bfloat16), jnp.sum(gates, axis=1)[:, None]


def shards(
    tokens, out_grad, expert_ids, route_gates, gate_weight, up_weight, down_weight, momentum
):
    token_count, model_width = tokens.shape
    topk_count = expert_ids.shape[1]
    peers, cores = lax.axis_size("ep"), lax.axis_size("opt")
    capacity = 2 * token_count * topk_count // peers
    slot_count = peers * capacity
    chosen, gates = placement(expert_ids, route_gates, slot_count, capacity)
    part = model_width // cores
    first = lax.axis_index("opt") * part
    part_tokens = lax.dynamic_slice_in_dim(tokens, first, part, 1)
    part_grads = lax.dynamic_slice_in_dim(out_grad, first, part, 1)
    send_inputs = jnp.dot(chosen, part_tokens, preferred_element_type=jnp.float32).astype(
        jnp.bfloat16
    )
    send_scaled = (
        gates * jnp.dot(chosen, part_grads, preferred_element_type=jnp.float32)
    ).astype(jnp.bfloat16)
    shape = (peers, capacity, part)
    recv_inputs, recv_scaled = dispatch(
        send_inputs.reshape(shape), send_scaled.reshape(shape), peers, cores
    )
    recv_inputs = recv_inputs.reshape(slot_count, model_width)
    recv_scaled = recv_scaled.reshape(slot_count, model_width)
    weight_gate = gate_weight[0]
    weight_up = up_weight[0]
    weight_down = down_weight[0]
    pre_gate = jnp.dot(recv_inputs, weight_gate, preferred_element_type=jnp.float32)
    pre_up = jnp.dot(recv_inputs, weight_up, preferred_element_type=jnp.float32)
    sigmoid = jax.nn.sigmoid(pre_gate)
    activated = pre_gate * sigmoid
    hidden = (activated * pre_up).astype(jnp.bfloat16)
    hidden_grad = lax.dot_general(
        recv_scaled, weight_down, CONTRACT_LAST, preferred_element_type=jnp.float32
    )
    gate_grad = (hidden_grad * pre_up * sigmoid * (1.0 + pre_gate * (1.0 - sigmoid))).astype(
        jnp.bfloat16
    )
    up_grad = (hidden_grad * activated).astype(jnp.bfloat16)
    partial_grad = lax.dot_general(
        gate_grad, weight_gate, CONTRACT_LAST, preferred_element_type=jnp.float32
    ) + lax.dot_general(up_grad, weight_up, CONTRACT_LAST, preferred_element_type=jnp.float32)
    partial_grad = partial_grad.astype(jnp.bfloat16).reshape(peers, capacity, model_width)
    down_grad = lax.dot_general(
        hidden, recv_scaled, CONTRACT_FIRST, preferred_element_type=jnp.float32
    )
    new_moment = momentum_decay * momentum[0] + down_grad
    squares = jnp.broadcast_to(jnp.sum(new_moment * new_moment), (8, 128))
    returned, own_rows = return_and_orthogonalize(partial_grad, new_moment, squares, cores)
    token_grad = lax.dot_general(
        chosen, returned.reshape(slot_count, part), CONTRACT_FIRST,
        preferred_element_type=jnp.float32,
    ).astype(jnp.bfloat16)
    update = math.sqrt(model_width) * own_rows.astype(jnp.float32)
    return (token_grad, new_moment[None], update[None])


def solution(mesh):
    in_specs = (
        P("ep", None),
        P("ep", None),
        P("ep", None),
        P("ep", None),
        P("ep", None, "opt"),
        P("ep", None, "opt"),
        P("ep", "opt", None),
        P("ep", "opt", None),
    )
    out_specs = (P("ep", "opt"), P("ep", "opt", None), P("ep", "opt", None))
    return jax.shard_map(shards, mesh=mesh, in_specs=in_specs, out_specs=out_specs, check_vma=False)
```
